32 devices in a mesh: dp: 2 (over z, core), sp: 16 (over x, y).
Axes of the slice: x: 4, y: 4, z: 1, core: 2. Of those that a mesh axis runs over, the one named last changes fastest.
The devices are a block of a 4x4x8 slice.
Arguments:
- x: bfloat16 [8192, 3072], P(('dp', 'sp')), parts along dimension 0
- gain: bfloat16 [3072], replicated
- wq: bfloat16 [3072, 4096], replicated
- wk: bfloat16 [3072, 4096], replicated
- wv: bfloat16 [3072, 4096], replicated
- wo: bfloat16 [4096, 3072], replicated
Outputs:
- output: bfloat16 [8192, 3072], P(('dp', 'sp')), parts along dimension 0
There are 2 independent parts. The reference program is written for one: setup_inputs(seed, part) draws one part's arguments, and reference() takes and returns one part's arrays. A program takes and returns all parts, laid end to end along the dimension named above; an argument that names none is the same for every part.
All inputs are finite; a program needn't handle non-finite values.
Results may differ from the reference program's by a relative error of at most 0.012.
Values are sent between devices in bfloat16 or wider.
A program may use at most 768 MiB of HBM per device.

```python
import jax
import jax.numpy as jnp
from jax import lax

ROWS = 4096
D = 3072
HEADS = 16
KV_HEADS = 16
HEAD = 256
THETA = 10000


def setup_inputs(seed: int = 0, part: int = 0) -> dict:
    kx, kn, kq, kk, kv, ko = jax.random.split(jax.random.key(seed), 6)

    def weights(key, rows, columns):
        return jax.random.normal(key, (rows, columns), jnp.float32) * rows**-0.5

    drawn = {
        "x": jax.random.normal(jax.random.fold_in(kx, part), (ROWS, D), jnp.float32),
        "gain": 1 + 0.1 * jax.random.normal(kn, (D,), jnp.float32),
        "wq": 2 * weights(kq, D, HEADS * HEAD),
        "wk": 2 * weights(kk, D, KV_HEADS * HEAD),
        "wv": 4 * weights(kv, D, KV_HEADS * HEAD),
        "wo": weights(ko, HEADS * HEAD, D),
    }
    return {k: v.astype(jnp.bfloat16) for k, v in drawn.items()}


def normed(x, gain):
    wide = x.astype(jnp.float32)
    scale = lax.rsqrt(jnp.mean(wide * wide, -1, keepdims=True) + 1e-6)
    return (wide * scale * gain.astype(jnp.float32)).astype(jnp.bfloat16)


def turned(t, place, theta):
    half = t.shape[-1] // 2
    angle = place.astype(jnp.float32)[:, None] * theta ** (-jnp.arange(half, dtype=jnp.float32) / half)
    cos, sin = jnp.cos(angle)[:, None], jnp.sin(angle)[:, None]
    a, b = t[..., :half].astype(jnp.float32), t[..., half:].astype(jnp.float32)
    return jnp.concatenate([a * cos - b * sin, b * cos + a * sin], -1).astype(jnp.bfloat16)


def matmul(a, w):
    return jnp.dot(a, w, preferred_element_type=jnp.float32).astype(jnp.bfloat16)


def einsum(form, a, b):
    return jnp.einsum(form, a.astype(jnp.float32), b.astype(jnp.float32))


def attention(q, k, v):
    scores = einsum("tgsd,ugd->gstu", q, k) * q.shape[-1] ** -0.5
    token = jnp.arange(q.shape[0])
    scores = jnp.where(token[:, None] >= token, scores, -jnp.inf)
    weights = jax.nn.softmax(scores, -1).astype(jnp.bfloat16)
    return einsum("gstu,ugd->tgsd", weights, v).astype(jnp.bfloat16)


def reference(x, gain, wq, wk, wv, wo):
    a, place = normed(x, gain), jnp.arange(ROWS)
    q = turned(matmul(a, wq).reshape(ROWS, HEADS, HEAD), place, THETA).reshape(ROWS, KV_HEADS, -1, HEAD)
    k = turned(matmul(a, wk).reshape(ROWS, KV_HEADS, HEAD), place, THETA)
    v = matmul(a, wv).reshape(ROWS, KV_HEADS, HEAD)
    seen = attention(q, k, v).reshape(ROWS, HEADS * HEAD)
    return (x.astype(jnp.float32) + jnp.dot(seen, wo, preferred_element_type=jnp.float32)).astype(jnp.bfloat16)
```

```python
import functools
import math

import jax
import jax.numpy as jnp
from jax import lax
from jax.experimental import pallas as pl
from jax.experimental.pallas import tpu as pltpu
from jax.sharding import PartitionSpec as P

HEAD = 256
THETA = 10000
LOG2E = 1.4426950408889634
MESH = pl.DeviceIdType.MESH
VMEM = 67_000_000
DEPTH = 4
WIDE = 1024


def _dot(a, b, ca, cb):
    return lax.dot_general(a, b, (((ca,), (cb,)), ((), ())), preferred_element_type=jnp.float32)


def _kernel(n, x_ref, gain_ref, cos_ref, sin_ref, wq_ref, wk_ref, wv_ref, wo_ref, y_ref,
            a_s, w_s, made_s, got_s, score_s, back_s, seen_s, wo_s, total_s,
            w_sem, send_sem, recv_sem, back_send_sem, back_recv_sem, wo_sem):
    side = math.isqrt(n)
    me = lax.axis_index("sp")
    mx, my = lax.div(me, side), lax.rem(me, side)
    own, d = x_ref.shape
    per = WIDE // own
    e = HEAD**-0.5 * LOG2E

    def at(s, sign):
        dx = lax.rem(s, side)
        dy = lax.rem(lax.div(s, side) + dx, side)
        return lax.rem(mx + sign * dx + side, side) * side + lax.rem(my + sign * dy + side, side)

    barrier = pltpu.get_barrier_semaphore()

    @pl.loop(1, n)
    def _(s):
        pl.semaphore_signal(barrier, inc=1, device_id={"sp": at(s, 1)}, device_id_type=MESH)

    sources = (wk_ref, wv_ref, wq_ref)

    def fetch(t, s, slot):
        head = pl.multiple_of(at(s, 1) * HEAD, HEAD)
        return pltpu.make_async_copy(sources[t].at[:, pl.ds(head, HEAD)], w_s.at[slot], w_sem.at[slot])

    for s in range(DEPTH - 1):
        fetch(0, s, s).start()

    wide = x_ref[...].astype(jnp.float32)
    scale = lax.rsqrt(jnp.mean(wide * wide, -1, keepdims=True) + 1e-6)
    a_s[...] = (wide * scale * gain_ref[...].astype(jnp.float32)).astype(jnp.bfloat16)

    pl.semaphore_wait(barrier, n - 1)

    def send(t, s):
        return pltpu.make_async_remote_copy(src_ref=made_s.at[t, s], dst_ref=got_s.at[t, me], send_sem=send_sem.at[t, s],
                                            recv_sem=recv_sem.at[t, s], device_id={"sp": at(s, 1)}, device_id_type=MESH)

    half = HEAD // 2
    for t in range(3):
        @pl.loop(0, n)
        def _(s, t=t):
            slot = lax.rem(s + t * n, DEPTH)
            ahead = lax.rem(s + t * n + DEPTH - 1, DEPTH)

            @pl.when(s < n - DEPTH + 1)
            def _():
                fetch(t, s + DEPTH - 1, ahead).start()

            if t < 2:
                @pl.when(s >= n - DEPTH + 1)
                def _():
                    fetch(t + 1, s + DEPTH - 1 - n, ahead).start()

            fetch(t, s, slot).wait()
            made = _dot(a_s[...], w_s[slot], 1, 0)
            if t == 1:
                out = made.astype(jnp.bfloat16)
            else:
                made = made.astype(jnp.bfloat16).astype(jnp.float32)
                u, v = made[:, :half], made[:, half:]
                c, sn = cos_ref[...], sin_ref[...]
                out = jnp.concatenate([u * c - v * sn, v * c + u * sn], -1).astype(jnp.bfloat16)

            @pl.when(s == 0)
            def _():
                got_s[t, me] = out

            @pl.when(s > 0)
            def _():
                made_s[t, s] = out
                send(t, s).start()

    def fetch_wo(h):
        rows = pl.ds(pl.multiple_of(h * HEAD, HEAD), HEAD)
        return pltpu.make_async_copy(wo_ref.at[rows, :], wo_s.at[rows, :], wo_sem.at[h])

    @pl.loop(0, n)
    def _(h):
        fetch_wo(h).start()

    for t in range(2):
        @pl.loop(1, n)
        def _(s, t=t):
            send(t, s).wait_recv()

    def back(s):
        return pltpu.make_async_remote_copy(src_ref=back_s.at[s], dst_ref=seen_s.at[s], send_sem=back_send_sem.at[s],
                                            recv_sem=back_recv_sem.at[s], device_id={"sp": at(s, -1)}, device_id_type=MESH)

    @pl.loop(0, n)
    def _(s):
        j = at(s, -1)

        @pl.when(s > 0)
        def _():
            send(2, s).wait_recv()

        q = got_s[2, j]
        last = lax.div(j, per)

        def keys(t, c):
            return got_s[t, pl.ds(c * per, per)].reshape(WIDE, HEAD)

        def peak(s, top):
            for i in range(0, WIDE, 128):
                top = jnp.maximum(top, s[:, i : i + 128])
            return top

        def score(c, top):
            got = _dot(q, keys(0, c), 1, 1)
            score_s[c] = got
            return peak(got, top)

        top = lax.fori_loop(0, last, score, jnp.full((own, 128), -jnp.inf, jnp.float32))
        got = _dot(q, keys(0, last), 1, 1)
        gap = lax.broadcasted_iota(jnp.int32, (own, WIDE), 0) - lax.broadcasted_iota(jnp.int32, (own, WIDE), 1)
        got = jnp.where(gap >= last * WIDE - j * own, got, -jnp.inf)
        score_s[last] = got
        top = jnp.max(peak(got, top), axis=1, keepdims=True)

        def weigh(c, carry):
            total, mix = carry
            p = jnp.exp2((score_s[c] - top) * e)
            for i in range(0, WIDE, 128):
                total = total + p[:, i : i + 128]
            return total, mix + _dot(p.astype(jnp.bfloat16), keys(1, c), 1, 0)

        total, mix = lax.fori_loop(0, last + 1, weigh, (jnp.zeros((own, 128), jnp.float32), jnp.zeros((own, HEAD), jnp.float32)))
        out = (mix / jnp.sum(total, axis=1, keepdims=True)).astype(jnp.bfloat16)

        @pl.when(s == 0)
        def _():
            seen_s[0] = out

        @pl.when(s > 0)
        def _():
            back_s[s] = out
            back(s).start()

    total_s[...] = x_ref[...].astype(jnp.float32)

    @pl.loop(0, n)
    def _(h):
        fetch_wo(h).wait()

    @pl.loop(0, n)
    def _(s):
        @pl.when(s > 0)
        def _():
            back(s).wait_recv()

        rows = pl.ds(pl.multiple_of(at(s, 1) * HEAD, HEAD), HEAD)
        for i in range(0, d, 512):
            total_s[:, i : i + 512] += _dot(seen_s[s], wo_s[rows, i : i + 512], 1, 0)

    y_ref[...] = total_s[...].astype(jnp.bfloat16)

    @pl.loop(1, n)
    def _(s):
        for t in range(3):
            send(t, s).wait_send()
        back(s).wait_send()


def solution(mesh):
    n = mesh.shape["sp"]

    def step(x, gain, wq, wk, wv, wo):
        own, d = x.shape
        place = lax.axis_index("sp") * own + jnp.arange(own)
        half = HEAD // 2
        angle = place.astype(jnp.float32)[:, None] * THETA ** (-jnp.arange(half, dtype=jnp.float32) / half)
        vmem, hbm = pl.BlockSpec(memory_space=pltpu.VMEM), pl.BlockSpec(memory_space=pl.ANY)
        low, wide = jnp.bfloat16, jnp.float32
        return pl.pallas_call(
            functools.partial(_kernel, n),
            out_shape=jax.ShapeDtypeStruct((own, d), low),
            in_specs=[vmem] * 4 + [hbm] * 4,
            out_specs=vmem,
            scratch_shapes=[
                pltpu.VMEM((own, d), low),
                pltpu.VMEM((DEPTH, d, HEAD), low),
                pltpu.VMEM((3, n, own, HEAD), low),
                pltpu.VMEM((3, n, own, HEAD), low),
                pltpu.VMEM((n * own // WIDE, own, WIDE), wide),
                pltpu.VMEM((n, own, HEAD), low),
                pltpu.VMEM((n, own, HEAD), low),
                pltpu.VMEM((n * HEAD, d), low),
                pltpu.VMEM((own, d), wide),
                pltpu.SemaphoreType.DMA((DEPTH,)),
                pltpu.SemaphoreType.DMA((3, n)),
                pltpu.SemaphoreType.DMA((3, n)),
                pltpu.SemaphoreType.DMA((n,)),
                pltpu.SemaphoreType.DMA((n,)),
                pltpu.SemaphoreType.DMA((n,)),
            ],
            compiler_params=pltpu.CompilerParams(collective_id=0, has_side_effects=True, vmem_limit_bytes=VMEM),
        )(x, gain[None], jnp.cos(angle), jnp.sin(angle), wq, wk, wv, wo)

    tokens, whole = P(("dp", "sp"), None), P(None, None)
    return jax.shard_map(
        step,
        mesh=mesh,
        in_specs=(tokens, P(None), whole, whole, whole, whole),
        out_specs=tokens,
        check_vma=False,
    )
```

```python
import functools
import math

import jax
import jax.numpy as jnp
from jax import lax
from jax.experimental import pallas as pl
from jax.experimental.pallas import tpu as pltpu
from jax.sharding import PartitionSpec as P

HEAD = 256
THETA = 10000
LOG2E = 1.4426950408889634
MESH = pl.DeviceIdType.MESH
VMEM = 66_500_000
WIDE = 1024
FINE = 16


def _dot(a, b, ca, cb):
    return lax.dot_general(a, b, (((ca,), (cb,)), ((), ())), preferred_element_type=jnp.float32)


def _kernel(n, x_ref, gain_ref, cos_ref, sin_ref, wq_ref, wk_ref, wv_ref, wo_ref, y_ref,
            a_s, w_s, made_s, got_s, score_s, seen_s, cos_s, sin_s,
            x_sem, w_sem, a_send, a_recv, send_sem, recv_sem, back_send, back_recv, wo_sem):
    side = math.isqrt(n)
    me = lax.axis_index("sp")
    mx, my = lax.div(me, side), lax.rem(me, side)
    own, d = x_ref.shape
    part = own // 2
    per = WIDE // own
    steps = n // per
    e = HEAD**-0.5 * LOG2E
    half = HEAD // 2

    def go(dx, dy):
        return lax.rem(mx + dx + side, side) * side + lax.rem(my + dy + side, side)

    def along(axis, hop):
        return go(hop * (1 - axis), hop * axis)

    def at(s, sign):
        dx = lax.rem(s, side)
        return go(sign * dx, sign * lax.rem(lax.div(s, side) + dx, side))

    take_x = pltpu.make_async_copy(x_ref, y_ref, x_sem.at[0])
    take_x.start()
    barrier = pltpu.get_barrier_semaphore()

    @pl.loop(1, n)
    def _(s):
        pl.semaphore_signal(barrier, inc=1, device_id={"sp": at(s, 1)}, device_id_type=MESH)

    slots = 2 * side - 1

    def slot(axis, hop):
        return hop + axis * (side - 1) * lax.min(hop, 1)

    def fetch(t, i):
        head = along(1, i) if i < side else along(0, i - side + 1)
        columns = pl.ds(pl.multiple_of(head * HEAD, HEAD), HEAD)
        return pltpu.make_async_copy((wk_ref, wv_ref, wq_ref)[t].at[:, columns], w_s.at[t * slots + i], w_sem.at[t * slots + i])

    for i in range(slots):
        for t in range(3):
            fetch(t, i).start()

    take_x.wait()
    wide = y_ref[...].astype(jnp.float32)
    scale = lax.rsqrt(jnp.mean(wide * wide, -1, keepdims=True) + 1e-6)
    a = (wide * scale * gain_ref[...].astype(jnp.float32)).astype(jnp.bfloat16)
    a_s[0, 0] = a[:part]
    a_s[1, 0] = a[part:]

    pl.semaphore_wait(barrier, n - 1)

    def spread(axis, way):
        return pltpu.make_async_remote_copy(
            src_ref=a_s.at[axis, 0], dst_ref=a_s.at[axis, 1 + way], send_sem=a_send.at[axis, way], recv_sem=a_recv.at[axis, way],
            device_id={"sp": along(axis, 1 - 2 * way)}, device_id_type=MESH)

    def relay(axis, way):
        rows = pl.ds(way * (part // 2), part // 2)
        return pltpu.make_async_remote_copy(
            src_ref=a_s.at[axis, 1 + way, rows], dst_ref=a_s.at[axis, 3, rows], send_sem=a_send.at[axis, 2 + way],
            recv_sem=a_recv.at[axis, 2 + way], device_id={"sp": along(axis, 1 - 2 * way)}, device_id_type=MESH)

    ways = [(axis, way) for way in range(2) for axis in range(2)]
    for axis, way in ways:
        spread(axis, way).start()

    for i in range(own // FINE):
        rows = slice(i * FINE, (i + 1) * FINE)
        c1, s1, c0, s0 = cos_ref[FINE + i : FINE + i + 1], sin_ref[FINE + i : FINE + i + 1], cos_ref[:FINE], sin_ref[:FINE]
        cos_s[rows] = c1 * c0 - s1 * s0
        sin_s[rows] = s1 * c0 + c1 * s0

    def send(axis, k, hop, t):
        block = along(axis, place(k))
        return pltpu.make_async_remote_copy(
            src_ref=made_s.at[axis, k, hop - 1, t], dst_ref=got_s.at[t, block, pl.ds(axis * part, part)], send_sem=send_sem.at[axis, k, hop, t],
            recv_sem=recv_sem.at[axis, k, hop, t], device_id={"sp": along(1 - axis, hop)}, device_id_type=MESH)

    def place(k):
        return lax.div(k, 2) * (k - 1) - lax.rem(k, 2) * (1 - lax.div(k, 2))

    @pl.loop(0, 2 * side)
    def _(g):
        axis, k = lax.rem(g, 2), lax.div(g, 2)

        @pl.when(g == 2)
        def _():
            for axis, way in ways:
                spread(axis, way).wait_recv()
                relay(axis, way).start()

        @pl.when(g == 6)
        def _():
            for axis, way in ways:
                relay(axis, way).wait_recv()

        block = along(axis, place(k))
        c1, s1 = cos_ref[pl.ds(2 * FINE + block, 1)], sin_ref[pl.ds(2 * FINE + block, 1)]
        here = pl.ds(pl.multiple_of(axis * part, part), part)
        c0, s0 = cos_s[here], sin_s[here]
        c, sn = c1 * c0 - s1 * s0, s1 * c0 + c1 * s0

        @pl.loop(0, side)
        def _(hop):
            for t in range(3):
                at_slot = t * slots + slot(axis, hop)

                @pl.when((g == 0) | ((g == 1) & (hop > 0)))
                def _():
                    pltpu.make_async_copy(wo_ref.at[pl.ds(0, d), pl.ds(0, HEAD)], w_s.at[at_slot], w_sem.at[at_slot]).wait()

                made = _dot(a_s[axis, k], w_s[at_slot], 1, 0).astype(jnp.bfloat16)
                if t != 1:
                    made = made.astype(jnp.float32)
                    u, v = made[:, :half], made[:, half:]
                    made = jnp.concatenate([u * c - v * sn, v * c + u * sn], -1).astype(jnp.bfloat16)

                @pl.when(hop == 0)
                def _():
                    got_s[t, block, here] = made

                @pl.when(hop > 0)
                def _():
                    made_s[axis, k, hop - 1, t] = made
                    send(axis, k, hop, t).start()

    def fetch_wo(h, i):
        rows = pl.ds(pl.multiple_of(h * HEAD, HEAD), HEAD)
        return pltpu.make_async_copy(wo_ref.at[rows, pl.ds(i * HEAD, HEAD)], w_s.at[h, pl.ds(i * HEAD, HEAD)], wo_sem.at[h, i])

    @pl.loop(0, n)
    def _(h):
        for i in range(d // HEAD):
            fetch_wo(h, i).start()

    @pl.loop(0, 2 * side)
    def _(g):
        @pl.loop(1, side)
        def _(hop):
            for t in range(3):
                send(lax.rem(g, 2), lax.div(g, 2), hop, t).wait_recv()

    def back(s):
        return pltpu.make_async_remote_copy(src_ref=got_s.at[2, at(s, -1)], dst_ref=seen_s.at[s], send_sem=back_send.at[s], recv_sem=back_recv.at[s],
                                            device_id={"sp": at(s, -1)}, device_id_type=MESH)

    def peak(top, s):
        for i in range(0, WIDE, 128):
            top = jnp.maximum(top, s[:, i : i + 128])
        return top

    def attend(s, j, last):
        keys = lambda t, c: got_s[t, c * per : (c + 1) * per].reshape(WIDE, HEAD)
        q = got_s[2, j]
        top = jnp.full((own, 128), -jnp.inf, jnp.float32)
        for c in range(last + 1):
            got = _dot(q, keys(0, c), 1, 1)
            if c == last:
                gap = lax.broadcasted_iota(jnp.int32, (own, WIDE), 0) - lax.broadcasted_iota(jnp.int32, (own, WIDE), 1)
                got = jnp.where(gap >= last * WIDE - j * own, got, -jnp.inf)
            score_s[c] = got
            top = peak(top, got)
        top = jnp.max(top, axis=1, keepdims=True)
        total, mix = jnp.zeros((own, 128), jnp.float32), jnp.zeros((own, HEAD), jnp.float32)
        for c in range(last + 1):
            p = jnp.exp2((score_s[c] - top) * e)
            for i in range(0, WIDE, 128):
                total = total + p[:, i : i + 128]
            mix = mix + _dot(p.astype(jnp.bfloat16), keys(1, c), 1, 0)
        out = (mix / jnp.sum(total, axis=1, keepdims=True)).astype(jnp.bfloat16)

        @pl.when(s == 0)
        def _():
            seen_s[0] = out

        @pl.when(s > 0)
        def _():
            got_s[2, j] = out

    @pl.loop(0, n)
    def _(s):
        j = at(s, -1)
        for last in range(steps):
            pl.when(lax.div(j, per) == last)(functools.partial(attend, s, j, last))

        @pl.when(s > 0)
        def _():
            back(s).start()

    runs = d // WIDE
    for i in range(runs):
        score_s[i] = y_ref[:, i * WIDE : (i + 1) * WIDE].astype(jnp.float32)

    @pl.loop(0, n)
    def _(h):
        for i in range(d // HEAD):
            fetch_wo(h, i).wait()

    @pl.loop(0, n)
    def _(s):
        @pl.when(s > 0)
        def _():
            back(s).wait_recv()

        h, seen = at(s, 1), seen_s[s]
        for i in range(d // HEAD):
            columns = slice(i * HEAD % WIDE, i * HEAD % WIDE + HEAD)
            score_s[i * HEAD // WIDE, :, columns] += _dot(seen, w_s[h, i * HEAD : (i + 1) * HEAD], 1, 0)

    for i in range(runs):
        y_ref[:, i * WIDE : (i + 1) * WIDE] = score_s[i].astype(jnp.bfloat16)

    for axis, way in ways:
        spread(axis, way).wait_send()
        relay(axis, way).wait_send()

    @pl.loop(0, 2 * side)
    def _(g):
        @pl.loop(1, side)
        def _(hop):
            for t in range(3):
                send(lax.rem(g, 2), lax.div(g, 2), hop, t).wait_send()

    @pl.loop(1, n)
    def _(s):
        back(s).wait_send()


def solution(mesh):
    n = mesh.shape["sp"]
    side = math.isqrt(n)

    def step(x, gain, wq, wk, wv, wo):
        own, d = x.shape
        half = HEAD // 2
        place = jnp.concatenate([jnp.arange(FINE), jnp.arange(FINE) * FINE, jnp.arange(n) * own])
        angle = place.astype(jnp.float32)[:, None] * THETA ** (-jnp.arange(half, dtype=jnp.float32) / half)
        vmem, hbm = pl.BlockSpec(memory_space=pltpu.VMEM), pl.BlockSpec(memory_space=pl.ANY)
        low, wide, dma = jnp.bfloat16, jnp.float32, pltpu.SemaphoreType.DMA
        slots = 3 * (2 * side - 1)
        return pl.pallas_call(
            functools.partial(_kernel, n),
            out_shape=jax.ShapeDtypeStruct((own, d), low),
            in_specs=[hbm] + [vmem] * 3 + [hbm] * 4,
            out_specs=vmem,
            scratch_shapes=[
                pltpu.VMEM((2, side, own // 2, d), low),
                pltpu.VMEM((slots, d, HEAD), low),
                pltpu.VMEM((2, side, side - 1, 3, own // 2, HEAD), low),
                pltpu.VMEM((3, n, own, HEAD), low),
                pltpu.VMEM((n * own // WIDE, own, WIDE), wide),
                pltpu.VMEM((n, own, HEAD), low),
                pltpu.VMEM((own, half), wide),
                pltpu.VMEM((own, half), wide),
                dma((1,)),
                dma((slots,)),
                dma((2, 4)),
                dma((2, 4)),
                dma((2, side, side, 3)),
                dma((2, side, side, 3)),
                dma((n,)),
                dma((n,)),
                dma((n, d // HEAD)),
            ],
            compiler_params=pltpu.CompilerParams(collective_id=0, has_side_effects=True, vmem_limit_bytes=VMEM),
        )(x, gain[None], jnp.cos(angle), jnp.sin(angle), wq, wk, wv, wo)

    tokens, whole = P(("dp", "sp"), None), P(None, None)
    return jax.shard_map(
        step,
        mesh=mesh,
        in_specs=(tokens, P(None), whole, whole, whole, whole),
        out_specs=tokens,
        check_vma=False,
    )
```

```python
import functools
import math

import jax
import jax.numpy as jnp
from jax import lax
from jax.experimental import pallas as pl
from jax.experimental.pallas import tpu as pltpu
from jax.sharding import PartitionSpec as P

HEAD = 256
THETA = 10000
LOG2E = 1.4426950408889634
MESH = pl.DeviceIdType.MESH
VMEM = 67_043_328
WIDE = 1024
PIECE = 512
FINE = 16


def _dot(a, b, ca, cb):
    return lax.dot_general(a, b, (((ca,), (cb,)), ((), ())), preferred_element_type=jnp.float32)


def _kernel(n, x_ref, gain_ref, cos_ref, sin_ref, wq_ref, wk_ref, wv_ref, wo_ref, y_ref,
            a_s, w_s, made_s, got_s, score_s, seen_s, cos_s, sin_s,
            x_sem, w_sem, a_send, a_recv, send_sem, recv_sem, back_send, back_recv, wo_sem):
    side = math.isqrt(n)
    me = lax.axis_index("sp")
    mx, my = lax.div(me, side), lax.rem(me, side)
    own, d = x_ref.shape
    part = own // 2
    per = WIDE // own
    e = HEAD**-0.5 * LOG2E
    half = HEAD // 2

    def go(dx, dy):
        return lax.rem(mx + dx + side, side) * side + lax.rem(my + dy + side, side)

    def along(axis, hop):
        return go(hop * (1 - axis), hop * axis)

    def at(s, sign):
        dx = lax.rem(s, side)
        return go(sign * dx, sign * lax.rem(lax.div(s, side) + dx, side))

    take_x = pltpu.make_async_copy(x_ref, y_ref, x_sem.at[0])
    take_x.start()
    barrier = pltpu.get_barrier_semaphore()

    @pl.loop(1, n)
    def _(s):
        pl.semaphore_signal(barrier, inc=1, device_id={"sp": at(s, 1)}, device_id_type=MESH)

    slots = 2 * side - 1

    def slot(axis, hop):
        return hop + axis * (side - 1) * lax.min(hop, 1)

    def fetch(t, i):
        head = along(1, i) if i < side else along(0, i - side + 1)
        columns = pl.ds(pl.multiple_of(head * HEAD, HEAD), HEAD)
        return pltpu.make_async_copy((wk_ref, wv_ref, wq_ref)[t].at[:, columns], w_s.at[t * slots + i], w_sem.at[t * slots + i])

    for i in range(slots):
        for t in range(3):
            fetch(t, i).start()

    take_x.wait()
    gain = gain_ref[...].astype(jnp.float32).reshape(1, d)

    @pl.loop(0, own // FINE)
    def _(i):
        wide = y_ref[pl.ds(pl.multiple_of(i * FINE, FINE), FINE)].astype(jnp.float32)
        scale = lax.rsqrt(jnp.mean(wide * wide, -1, keepdims=True) + 1e-6)
        at_row = lax.rem(i, part // FINE) * FINE
        a_s[lax.div(i, part // FINE), 0, pl.ds(pl.multiple_of(at_row, FINE), FINE)] = (wide * scale * gain).astype(jnp.bfloat16)

    pl.semaphore_wait(barrier, n - 1)

    def spread(axis, way):
        return pltpu.make_async_remote_copy(
            src_ref=a_s.at[axis, 0], dst_ref=a_s.at[axis, 1 + way], send_sem=a_send.at[axis, way], recv_sem=a_recv.at[axis, way],
            device_id={"sp": along(axis, 1 - 2 * way)}, device_id_type=MESH)

    def relay(axis, way):
        rows = pl.ds(way * (part // 2), part // 2)
        return pltpu.make_async_remote_copy(
            src_ref=a_s.at[axis, 1 + way, rows], dst_ref=a_s.at[axis, 3, rows], send_sem=a_send.at[axis, 2 + way],
            recv_sem=a_recv.at[axis, 2 + way], device_id={"sp": along(axis, 1 - 2 * way)}, device_id_type=MESH)

    ways = [(axis, way) for way in range(2) for axis in range(2)]
    for axis, way in ways:
        spread(axis, way).start()

    for i in range(own // FINE):
        rows = slice(i * FINE, (i + 1) * FINE)
        c1, s1, c0, s0 = cos_ref[FINE + i : FINE + i + 1], sin_ref[FINE + i : FINE + i + 1], cos_ref[:FINE], sin_ref[:FINE]
        cos_s[rows] = c1 * c0 - s1 * s0
        sin_s[rows] = s1 * c0 + c1 * s0

    def send(axis, k, hop, t):
        block = along(axis, place(k))
        return pltpu.make_async_remote_copy(
            src_ref=made_s.at[axis, lax.rem(k, side - 1), hop - 1, t], dst_ref=got_s.at[t, block, pl.ds(axis * part, part)], send_sem=send_sem.at[axis, k, hop, t],
            recv_sem=recv_sem.at[axis, k, hop, t], device_id={"sp": along(1 - axis, hop)}, device_id_type=MESH)

    def place(k):
        return lax.div(k, 2) * (k - 1) - lax.rem(k, 2) * (1 - lax.div(k, 2))

    def project(places):
        @pl.loop(0, 2 * side)
        def _(i):
            axis, hop = lax.div(i, side), lax.rem(i, side)
            ats = [t * slots + slot(axis, hop) for t in range(3)]

            if places == (0,):
                @pl.when((axis == 0) | (hop > 0))
                def _():
                    for at_slot in ats:
                        pltpu.make_async_copy(wo_ref.at[pl.ds(0, d), pl.ds(0, HEAD)], w_s.at[at_slot], w_sem.at[at_slot]).wait()

            here = pl.ds(pl.multiple_of(axis * part, part), part)
            c0, s0 = cos_s[here], sin_s[here]
            blocks = [along(axis, place(k)) for k in places]
            turns = [(cos_ref[pl.ds(2 * FINE + block, 1)], sin_ref[pl.ds(2 * FINE + block, 1)]) for block in blocks]
            c = jnp.concatenate([c1 * c0 - s1 * s0 for c1, s1 in turns], 0)
            sn = jnp.concatenate([s1 * c0 + c1 * s0 for c1, s1 in turns], 0)
            normed = a_s[axis, places[0] : places[-1] + 1].reshape(len(places) * part, d)
            room = lax.max(hop - 1, 0)
            for t in range(3):
                made = _dot(normed, w_s[ats[t]], 1, 0).astype(jnp.bfloat16)
                if t != 1:
                    made = made.astype(jnp.float32)
                    u, v = made[:, :half], made[:, half:]
                    made = jnp.concatenate([u * c - v * sn, v * c + u * sn], -1).astype(jnp.bfloat16)
                for i, k in enumerate(places):
                    made_s[axis, k % (side - 1), room, t] = made[i * part : (i + 1) * part]

            @pl.when(hop == 0)
            def _():
                for k, block in zip(places, blocks):
                    for t in range(3):
                        got_s[t, block, here] = made_s[axis, k % (side - 1), room, t]

            @pl.when(hop > 0)
            def _():
                for k in places:
                    for t in range(3):
                        send(axis, k, hop, t).start()

    project((0,))
    for axis, way in ways:
        spread(axis, way).wait_recv()
        relay(axis, way).start()
    project((1, 2))
    for axis, way in ways:
        relay(axis, way).wait_recv()

    def sent(k):
        for axis in range(2):
            @pl.loop(1, side)
            def _(hop, axis=axis):
                for t in range(3):
                    send(axis, k, hop, t).wait_send()

    sent(0)
    project((3,))

    def fetch_wo(h, i):
        rows = pl.ds(pl.multiple_of(h * HEAD, HEAD), HEAD)
        return pltpu.make_async_copy(wo_ref.at[rows, pl.ds(i * HEAD, HEAD)], w_s.at[h, pl.ds(i * HEAD, HEAD)], wo_sem.at[h, i])

    @pl.loop(0, n)
    def _(h):
        for i in range(d // HEAD):
            fetch_wo(h, i).start()

    @pl.loop(0, 2 * side)
    def _(g):
        @pl.loop(1, side)
        def _(hop):
            for t in range(3):
                send(lax.rem(g, 2), lax.div(g, 2), hop, t).wait_recv()

    def back(j, h):
        return pltpu.make_async_remote_copy(src_ref=got_s.at[2, j], dst_ref=seen_s.at[h], send_sem=back_send.at[j], recv_sem=back_recv.at[h],
                                            device_id={"sp": j}, device_id_type=MESH)

    def pair(s, sign):
        dx = lax.rem(s, side)
        dy = sign * (lax.div(s, side) + dx)
        return lax.rem(mx + sign * dx + side, side) * side + 2 * lax.rem(lax.div(my, 2) + dy + 4 * side, side // 2)

    def attend(j):
        rows, last = 2 * own, lax.div(j, per)
        q = got_s[2, pl.ds(j, 2)].reshape(rows, HEAD)

        def keys(t, c, i):
            return got_s[t, pl.ds(c * per + i * PIECE // own, PIECE // own)].reshape(PIECE, HEAD)

        def score(c, top, masked=False):
            for i in range(WIDE // PIECE):
                got = _dot(q, keys(0, c, i), 1, 1)
                if masked:
                    gap = lax.broadcasted_iota(jnp.int32, (rows, PIECE), 0) - lax.broadcasted_iota(jnp.int32, (rows, PIECE), 1)
                    got = jnp.where(gap >= c * WIDE + i * PIECE - j * own, got, -jnp.inf)
                score_s[c, :, i * PIECE : (i + 1) * PIECE] = got
                for x in range(0, PIECE, 128):
                    top = jnp.maximum(top, got[:, x : x + 128])
            return top

        top = lax.fori_loop(0, last, score, jnp.full((rows, 128), -jnp.inf, jnp.float32))
        top = jnp.max(score(last, top, True), axis=1, keepdims=True)

        def weigh(c, carry):
            total, mix = carry
            for i in range(WIDE // PIECE):
                p = jnp.exp2((score_s[c, :, i * PIECE : (i + 1) * PIECE] - top) * e)
                for x in range(0, PIECE, 128):
                    total = total + p[:, x : x + 128]
                mix = mix + _dot(p.astype(jnp.bfloat16), keys(1, c, i), 1, 0)
            return total, mix

        total, mix = lax.fori_loop(0, last + 1, weigh, (jnp.zeros((rows, 128), jnp.float32), jnp.zeros((rows, HEAD), jnp.float32)))
        out = mix / jnp.sum(total, axis=1, keepdims=True)
        got_s[2, pl.ds(j, 2)] = out.astype(jnp.bfloat16).reshape(2, own, HEAD)

    @pl.loop(0, n // 2)
    def _(s):
        j = pair(s, 1)
        attend(j)

        for i in range(2):
            @pl.when(j + i != me)
            def _():
                back(j + i, me).start()

    seen_s[me] = got_s[2, me]
    for i in range(d // WIDE):
        score_s[i, :own] = y_ref[:, i * WIDE : (i + 1) * WIDE].astype(jnp.float32)

    @pl.loop(0, n)
    def _(h):
        for i in range(d // HEAD):
            fetch_wo(h, i).wait()

    @pl.loop(0, n // 2)
    def _(s):
        h = pair(s, -1)
        for i in range(2):
            @pl.when(h + i != me)
            def _():
                back(me, h + i).wait_recv()

        for i in range(0, d, HEAD):
            score_s[i // WIDE, :own, i % WIDE : i % WIDE + HEAD] += _dot(seen_s[h], w_s[h, i : i + HEAD], 1, 0) + _dot(seen_s[h + 1], w_s[h + 1, i : i + HEAD], 1, 0)

    for i in range(d // WIDE):
        y_ref[:, i * WIDE : (i + 1) * WIDE] = score_s[i, :own].astype(jnp.bfloat16)

    for axis, way in ways:
        spread(axis, way).wait_send()
        relay(axis, way).wait_send()

    for k in range(1, side):
        sent(k)

    @pl.loop(0, n)
    def _(j):
        @pl.when(j != me)
        def _():
            back(j, me).wait_send()


def solution(mesh):
    n = mesh.shape["sp"]
    side = math.isqrt(n)

    def step(x, gain, wq, wk, wv, wo):
        own, d = x.shape
        half = HEAD // 2
        place = jnp.concatenate([jnp.arange(FINE), jnp.arange(FINE) * FINE, jnp.arange(n) * own])
        angle = place.astype(jnp.float32)[:, None] * THETA ** (-jnp.arange(half, dtype=jnp.float32) / half)
        vmem, hbm = pl.BlockSpec(memory_space=pltpu.VMEM), pl.BlockSpec(memory_space=pl.ANY)
        low, wide, dma = jnp.bfloat16, jnp.float32, pltpu.SemaphoreType.DMA
        slots = 3 * (2 * side - 1)
        return pl.pallas_call(
            functools.partial(_kernel, n),
            out_shape=jax.ShapeDtypeStruct((own, d), low),
            in_specs=[hbm] + [vmem] * 3 + [hbm] * 4,
            out_specs=vmem,
            scratch_shapes=[
                pltpu.VMEM((2, side, own // 2, d), low),
                pltpu.VMEM((slots, d, HEAD), low),
                pltpu.VMEM((2, side - 1, side - 1, 3, own // 2, HEAD), low),
                pltpu.VMEM((3, n, own, HEAD), low),
                pltpu.VMEM((n * own // WIDE, 2 * own, WIDE), wide),
                pltpu.VMEM((n, own, HEAD), low),
                pltpu.VMEM((own, half), wide),
                pltpu.VMEM((own, half), wide),
                dma((1,)),
                dma((slots,)),
                dma((2, 4)),
                dma((2, 4)),
                dma((2, side, side, 3)),
                dma((2, side, side, 3)),
                dma((n,)),
                dma((n,)),
                dma((n, d // HEAD)),
            ],
            compiler_params=pltpu.CompilerParams(collective_id=0, has_side_effects=True, vmem_limit_bytes=VMEM),
        )(x, gain, jnp.cos(angle), jnp.sin(angle), wq, wk, wv, wo)

    tokens, whole = P(("dp", "sp"), None), P(None, None)
    return jax.shard_map(
        step,
        mesh=mesh,
        in_specs=(tokens, P(None), whole, whole, whole, whole),
        out_specs=tokens,
        check_vma=False,
    )
```

```python
import functools
import math

import jax
import jax.numpy as jnp
from jax import lax
from jax.experimental import pallas as pl
from jax.experimental.pallas import tpu as pltpu
from jax.sharding import PartitionSpec as P

HEAD = 256
THETA = 10000
LOG2E = 1.4426950408889634
MESH = pl.DeviceIdType.MESH
VMEM = 67_043_328
PIECE = 512
FINE = 16


def _dot(a, b, ca, cb):
    return lax.dot_general(a, b, (((ca,), (cb,)), ((), ())), preferred_element_type=jnp.float32)


def _kernel(n, x_ref, gain_ref, cos_ref, sin_ref, wq_ref, wk_ref, wv_ref, wo_ref, y_ref,
            a_s, w_s, made_s, ask_s, got_s, score_s, seen_s, cos_s, sin_s,
            x_sem, w_sem, a_send, a_recv, send_sem, recv_sem, back_send, back_recv, wo_sem):
    side = math.isqrt(n)
    me = lax.axis_index("sp")
    mx, my = lax.div(me, side), lax.rem(me, side)
    own, d = x_ref.shape
    part = own // 2
    e = HEAD**-0.5 * LOG2E
    half = HEAD // 2

    def go(dx, dy):
        return lax.rem(mx + dx + side, side) * side + lax.rem(my + dy + side, side)

    def along(axis, hop):
        return go(hop * (1 - axis), hop * axis)

    def at(s, sign):
        dx = lax.rem(s, side)
        return go(sign * dx, sign * lax.rem(lax.div(s, side) + dx, side))

    take_x = pltpu.make_async_copy(x_ref, y_ref, x_sem.at[0])
    take_x.start()
    barrier = pltpu.get_barrier_semaphore()

    @pl.loop(1, n)
    def _(s):
        pl.semaphore_signal(barrier, inc=1, device_id={"sp": at(s, 1)}, device_id_type=MESH)

    slots = 2 * side - 1

    def slot(axis, hop):
        return hop + axis * (side - 1) * lax.min(hop, 1)

    def fetch(t, i):
        head = along(1, i) if i < side else along(0, i - side + 1)
        columns = pl.ds(pl.multiple_of(head * HEAD, HEAD), HEAD)
        return pltpu.make_async_copy((wk_ref, wv_ref, wq_ref)[t].at[:, columns], w_s.at[t * slots + i], w_sem.at[t * slots + i])

    for tensors in ((0, 1), (2,)):
        for i in (0, *range(1, side - 2), side - 1, side - 2, *range(side, slots)):
            for t in tensors:
                fetch(t, i).start()

    take_x.wait()
    gain = gain_ref[...].astype(jnp.float32).reshape(1, d)

    @pl.loop(0, own // FINE)
    def _(i):
        wide = y_ref[pl.ds(pl.multiple_of(i * FINE, FINE), FINE)].astype(jnp.float32)
        scale = lax.rsqrt(jnp.mean(wide * wide, -1, keepdims=True) + 1e-6)
        at_row = lax.rem(i, part // FINE) * FINE
        a_s[lax.div(i, part // FINE), 0, pl.ds(pl.multiple_of(at_row, FINE), FINE)] = (wide * scale * gain).astype(jnp.bfloat16)

    pl.semaphore_wait(barrier, n - 1)

    def spread(axis, way):
        return pltpu.make_async_remote_copy(
            src_ref=a_s.at[axis, 0], dst_ref=a_s.at[axis, 1 + way], send_sem=a_send.at[axis, way], recv_sem=a_recv.at[axis, way],
            device_id={"sp": along(axis, 1 - 2 * way)}, device_id_type=MESH)

    def relay(axis, way):
        rows = pl.ds(way * (part // 2), part // 2)
        return pltpu.make_async_remote_copy(
            src_ref=a_s.at[axis, 1 + way, rows], dst_ref=a_s.at[axis, 3, rows], send_sem=a_send.at[axis, 2 + way],
            recv_sem=a_recv.at[axis, 2 + way], device_id={"sp": along(axis, 1 - 2 * way)}, device_id_type=MESH)

    ways = [(axis, way) for way in range(2) for axis in range(2)]
    for axis, way in ways:
        spread(axis, way).start()

    for i in range(own // FINE):
        rows = slice(i * FINE, (i + 1) * FINE)
        c1, s1, c0, s0 = cos_ref[FINE + i : FINE + i + 1], sin_ref[FINE + i : FINE + i + 1], cos_ref[:FINE], sin_ref[:FINE]
        cos_s[rows] = c1 * c0 - s1 * s0
        sin_s[rows] = s1 * c0 + c1 * s0

    def send(axis, k, hop, t):
        block = along(axis, place(k))
        made = ask_s.at[axis, k, hop - 1] if t == 2 else made_s.at[axis, lax.rem(k, side - 1), hop - 1, t]
        return pltpu.make_async_remote_copy(
            src_ref=made, dst_ref=got_s.at[t, block, pl.ds(axis * part, part)], send_sem=send_sem.at[axis, k, hop, t],
            recv_sem=recv_sem.at[axis, k, hop, t], device_id={"sp": along(1 - axis, hop)}, device_id_type=MESH)

    def place(k):
        return lax.div(k, 2) * (k - 1) - lax.rem(k, 2) * (1 - lax.div(k, 2))

    def project(places, tensors):
        @pl.loop(0, 2 * side)
        def _(i):
            axis = lax.rem(i, 2) if tensors == (2,) else lax.div(i, side)
            hop = lax.div(i, 2) if tensors == (2,) else lax.rem(i, side)
            hop = hop + lax.div(hop, 2) * (5 - 2 * hop)

            if places[0] == 0:
                @pl.when((axis == 0) | (hop > 0))
                def _():
                    for t in tensors:
                        at_slot = t * slots + slot(axis, hop)
                        pltpu.make_async_copy(wo_ref.at[pl.ds(0, d), pl.ds(0, HEAD)], w_s.at[at_slot], w_sem.at[at_slot]).wait()

            here = pl.ds(pl.multiple_of(axis * part, part), part)
            c0, s0 = cos_s[here], sin_s[here]
            blocks = [along(axis, place(k)) for k in places]
            turns = [(cos_ref[pl.ds(2 * FINE + block, 1)], sin_ref[pl.ds(2 * FINE + block, 1)]) for block in blocks]
            c = jnp.concatenate([c1 * c0 - s1 * s0 for c1, s1 in turns], 0)
            sn = jnp.concatenate([s1 * c0 + c1 * s0 for c1, s1 in turns], 0)
            normed = a_s[axis, places[0] : places[-1] + 1].reshape(len(places) * part, d)
            room = lax.max(hop - 1, 0)

            def spot(k, t):
                return ask_s.at[axis, k, room] if t == 2 else made_s.at[axis, k % (side - 1), room, t]

            for t in tensors:
                made = _dot(normed, w_s[t * slots + slot(axis, hop)], 1, 0).astype(jnp.bfloat16)
                if t != 1:
                    made = made.astype(jnp.float32)
                    u, v = made[:, :half], made[:, half:]
                    made = jnp.concatenate([u * c - v * sn, v * c + u * sn], -1).astype(jnp.bfloat16)
                for i, k in enumerate(places):
                    spot(k, t)[...] = made[i * part : (i + 1) * part]

            @pl.when(hop == 0)
            def _():
                for k, block in zip(places, blocks):
                    for t in tensors:
                        got_s[t, block, here] = spot(k, t)[...]

            @pl.when(hop > 0)
            def _():
                for k in places:
                    for t in tensors:
                        send(axis, k, hop, t).start()

    project((0,), (0, 1))
    for axis, way in ways:
        spread(axis, way).wait_recv()
        relay(axis, way).start()
    project((1, 2), (0, 1))
    for axis, way in ways:
        relay(axis, way).wait_recv()

    def sent(k, tensors):
        for axis in range(2):
            @pl.loop(1, side)
            def _(hop, axis=axis):
                for t in tensors:
                    send(axis, k, hop, t).wait_send()

    sent(0, (0, 1))
    project((3,), (0, 1))
    project(tuple(range(side)), (2,))

    def fetch_wo(h, i):
        rows = pl.ds(pl.multiple_of(h * HEAD, HEAD), HEAD)
        return pltpu.make_async_copy(wo_ref.at[rows, pl.ds(i * HEAD, HEAD)], w_s.at[h, pl.ds(i * HEAD, HEAD)], wo_sem.at[h, i])

    @pl.loop(0, n)
    def _(h):
        for i in range(d // HEAD):
            fetch_wo(h, i).start()

    @pl.loop(0, 2 * side)
    def _(g):
        @pl.loop(1, side)
        def _(hop):
            for t in range(2):
                send(lax.rem(g, 2), lax.div(g, 2), hop, t).wait_recv()

    def back(j, h):
        return pltpu.make_async_remote_copy(src_ref=got_s.at[2, j], dst_ref=seen_s.at[h], send_sem=back_send.at[j], recv_sem=back_recv.at[h],
                                            device_id={"sp": j}, device_id_type=MESH)

    def pair(s, sign):
        r, end = lax.rem(s, 3), lax.div(s, 6)
        dx = (1 + 2 * r - 3 * lax.div(r, 2)) * (1 - end)
        other = lax.rem(lax.div(s, 3) + end * (side * 2 - 1 - s), 2)
        return lax.rem(mx + sign * dx + side, side) * side + 2 * lax.rem(lax.div(my, 2) + other, side // 2)

    def await_queries(block):
        dx, dy = lax.rem(lax.div(block, side) - mx + side, side), lax.rem(lax.rem(block, side) - my + side, side)
        for axis, here, there in ((0, dx, dy), (1, dy, dx)):
            hop = lax.rem(side - there, side)

            @pl.when(hop > 0)
            def _():
                send(axis, lax.rem(2 * here - lax.div(here, 2), side), hop, 2).wait_recv()

    def attend(j):
        rows = 2 * own
        q = got_s[2, pl.ds(j, 2)].reshape(rows, HEAD)
        whole, twos, odd = lax.div(j, 2), lax.div(j, 4), lax.rem(lax.div(j, 2), 2)

        def keys(t, c):
            return got_s[t, pl.ds(2 * c, 2)].reshape(PIECE, HEAD)

        def score(c, top, masked=False):
            got = _dot(q, keys(0, c), 1, 1)
            if masked:
                got = jnp.where(lax.broadcasted_iota(jnp.int32, (rows, PIECE), 0) >= lax.broadcasted_iota(jnp.int32, (rows, PIECE), 1), got, -jnp.inf)
            score_s[c] = got
            for x in range(0, PIECE, 128):
                top = jnp.maximum(top, got[:, x : x + 128])
            return top

        top = jnp.full((rows, 128), -jnp.inf, jnp.float32)
        top = lax.fori_loop(0, twos, lambda c, top: score(2 * c + 1, score(2 * c, top)), top)
        top = lax.fori_loop(2 * twos, whole, score, top)
        top = jnp.max(score(whole, top, True), axis=1, keepdims=True)

        def weigh(c, carry):
            total, mix = carry
            p = jnp.exp2((score_s[c] - top) * e)
            for x in range(0, PIECE, 128):
                total = total + p[:, x : x + 128]
            return total, mix + _dot(p.astype(jnp.bfloat16), keys(1, c), 1, 0)

        carry = jnp.zeros((rows, 128), jnp.float32), jnp.zeros((rows, HEAD), jnp.float32)
        carry = lax.fori_loop(0, twos, lambda c, carry: weigh(2 * c + 1, weigh(2 * c, carry)), carry)
        total, mix = lax.fori_loop(2 * twos, whole + 1, weigh, carry)
        out = mix / jnp.sum(total, axis=1, keepdims=True)
        got_s[2, pl.ds(j, 2)] = out.astype(jnp.bfloat16).reshape(2, own, HEAD)

    @pl.loop(0, n // 2)
    def _(s):
        j = pair(s, 1)
        for i in range(2):
            await_queries(j + i)
        attend(j)

        for i in range(2):
            @pl.when(j + i != me)
            def _():
                back(j + i, me).start()

    seen_s[me] = got_s[2, me]
    for i in range(d // PIECE):
        score_s[i, :own] = y_ref[:, i * PIECE : (i + 1) * PIECE].astype(jnp.float32)

    @pl.loop(0, n)
    def _(h):
        for i in range(d // HEAD):
            fetch_wo(h, i).wait()

    @pl.loop(0, n // 2)
    def _(s):
        h = pair(s, -1)
        for i in range(2):
            @pl.when(h + i != me)
            def _():
                back(me, h + i).wait_recv()

        for i in range(0, d, HEAD):
            score_s[i // PIECE, :own, i % PIECE : i % PIECE + HEAD] += _dot(seen_s[h], w_s[h, i : i + HEAD], 1, 0) + _dot(seen_s[h + 1], w_s[h + 1, i : i + HEAD], 1, 0)

    for i in range(d // PIECE):
        y_ref[:, i * PIECE : (i + 1) * PIECE] = score_s[i, :own].astype(jnp.bfloat16)

    for axis, way in ways:
        spread(axis, way).wait_send()
        relay(axis, way).wait_send()

    for k in range(side):
        sent(k, (0, 1, 2) if k else (2,))

    @pl.loop(0, n)
    def _(j):
        @pl.when(j != me)
        def _():
            back(j, me).wait_send()


def solution(mesh):
    n = mesh.shape["sp"]
    side = math.isqrt(n)

    def step(x, gain, wq, wk, wv, wo):
        own, d = x.shape
        half = HEAD // 2
        place = jnp.concatenate([jnp.arange(FINE), jnp.arange(FINE) * FINE, jnp.arange(n) * own])
        angle = place.astype(jnp.float32)[:, None] * THETA ** (-jnp.arange(half, dtype=jnp.float32) / half)
        vmem, hbm = pl.BlockSpec(memory_space=pltpu.VMEM), pl.BlockSpec(memory_space=pl.ANY)
        low, wide, dma = jnp.bfloat16, jnp.float32, pltpu.SemaphoreType.DMA
        slots = 3 * (2 * side - 1)
        return pl.pallas_call(
            functools.partial(_kernel, n),
            out_shape=jax.ShapeDtypeStruct((own, d), low),
            in_specs=[hbm] + [vmem] * 3 + [hbm] * 4,
            out_specs=vmem,
            scratch_shapes=[
                pltpu.VMEM((2, side, own // 2, d), low),
                pltpu.VMEM((slots, d, HEAD), low),
                pltpu.VMEM((2, side - 1, side - 1, 2, own // 2, HEAD), low),
                pltpu.VMEM((2, side, side - 1, own // 2, HEAD), low),
                pltpu.VMEM((3, n, own, HEAD), low),
                pltpu.VMEM((n * own // PIECE, 2 * own, PIECE), wide),
                pltpu.VMEM((n, own, HEAD), low),
                pltpu.VMEM((own, half), wide),
                pltpu.VMEM((own, half), wide),
                dma((1,)),
                dma((slots,)),
                dma((2, 4)),
                dma((2, 4)),
                dma((2, side, side, 3)),
                dma((2, side, side, 3)),
                dma((n,)),
                dma((n,)),
                dma((n, d // HEAD)),
            ],
            compiler_params=pltpu.CompilerParams(collective_id=0, has_side_effects=True, vmem_limit_bytes=VMEM),
        )(x, gain, jnp.cos(angle), jnp.sin(angle), wq, wk, wv, wo)

    tokens, whole = P(("dp", "sp"), None), P(None, None)
    return jax.shard_map(
        step,
        mesh=mesh,
        in_specs=(tokens, P(None), whole, whole, whole, whole),
        out_specs=tokens,
        check_vma=False,
    )
```

```python
import functools
import math

import jax
import jax.numpy as jnp
from jax import lax
from jax.experimental import pallas as pl
from jax.experimental.pallas import tpu as pltpu
from jax.sharding import PartitionSpec as P

HEAD = 256
THETA = 10000
LOG2E = 1.4426950408889634
MESH = pl.DeviceIdType.MESH
VMEM = 65_470_000
PIECE = 512
FINE = 16


def _dot(a, b, ca, cb):
    return lax.dot_general(a, b, (((ca,), (cb,)), ((), ())), preferred_element_type=jnp.float32)


def _kernel(n, x_ref, gain_ref, cos_ref, sin_ref, wq_ref, wk_ref, wv_ref, wo_ref, y_ref,
            a_s, w_s, made_s, ask_s, got_s, score_s, seen_s, cos_s, sin_s,
            x_sem, w_sem, a_send, a_recv, send_sem, recv_sem, back_send, back_recv, wo_sem):
    side = math.isqrt(n)
    me = lax.axis_index("sp")
    mx, my = lax.div(me, side), lax.rem(me, side)
    own, d = x_ref.shape
    part = own // 2
    e = HEAD**-0.5 * LOG2E
    half = HEAD // 2

    def go(dx, dy):
        return lax.rem(mx + dx + side, side) * side + lax.rem(my + dy + side, side)

    def along(axis, hop):
        return go(hop * (1 - axis), hop * axis)

    def at(s, sign):
        dx = lax.rem(s, side)
        return go(sign * dx, sign * lax.rem(lax.div(s, side) + dx, side))

    take_x = pltpu.make_async_copy(x_ref, y_ref, x_sem.at[0])
    take_x.start()
    barrier = pltpu.get_barrier_semaphore()

    @pl.loop(1, n)
    def _(s):
        pl.semaphore_signal(barrier, inc=1, device_id={"sp": at(s, 1)}, device_id_type=MESH)

    slots = 2 * side - 1

    def slot(axis, hop):
        return hop + axis * (side - 1) * lax.min(hop, 1)

    def fetch(t, i):
        head = along(1, i) if i < side else along(0, i - side + 1)
        columns = pl.ds(pl.multiple_of(head * HEAD, HEAD), HEAD)
        return pltpu.make_async_copy((wk_ref, wv_ref, wq_ref)[t].at[:, columns], w_s.at[t * slots + i], w_sem.at[t * slots + i])

    for tensors in ((0, 1), (2,)):
        for i in (0, *range(1, side - 2), side - 1, side - 2, *range(side, slots)):
            for t in tensors:
                fetch(t, i).start()

    take_x.wait()
    gain = gain_ref[...].astype(jnp.float32).reshape(1, d)

    @pl.loop(0, own // FINE)
    def _(i):
        wide = y_ref[pl.ds(pl.multiple_of(i * FINE, FINE), FINE)].astype(jnp.float32)
        scale = lax.rsqrt(jnp.mean(wide * wide, -1, keepdims=True) + 1e-6)
        at_row = lax.rem(i, part // FINE) * FINE
        a_s[lax.div(i, part // FINE), 0, pl.ds(pl.multiple_of(at_row, FINE), FINE)] = (wide * scale * gain).astype(jnp.bfloat16)

    pl.semaphore_wait(barrier, n - 1)

    def spread(axis, way):
        return pltpu.make_async_remote_copy(
            src_ref=a_s.at[axis, 0], dst_ref=a_s.at[axis, 1 + way], send_sem=a_send.at[axis, way], recv_sem=a_recv.at[axis, way],
            device_id={"sp": along(axis, 1 - 2 * way)}, device_id_type=MESH)

    def relay(axis, way):
        rows = pl.ds(way * (part // 2), part // 2)
        return pltpu.make_async_remote_copy(
            src_ref=a_s.at[axis, 1 + way, rows], dst_ref=a_s.at[axis, 3, rows], send_sem=a_send.at[axis, 2 + way],
            recv_sem=a_recv.at[axis, 2 + way], device_id={"sp": along(axis, 1 - 2 * way)}, device_id_type=MESH)

    ways = [(axis, way) for way in range(2) for axis in range(2)]
    for axis, way in ways:
        spread(axis, way).start()

    for i in range(own // FINE):
        rows = slice(i * FINE, (i + 1) * FINE)
        c1, s1, c0, s0 = cos_ref[FINE + i : FINE + i + 1], sin_ref[FINE + i : FINE + i + 1], cos_ref[:FINE], sin_ref[:FINE]
        cos_s[rows] = c1 * c0 - s1 * s0
        sin_s[rows] = s1 * c0 + c1 * s0

    def send(axis, k, hop, t):
        block = along(axis, place(k))
        made = ask_s.at[axis, k, hop - 1] if t == 2 else made_s.at[axis, lax.rem(k, side - 1), hop - 1, t]
        return pltpu.make_async_remote_copy(
            src_ref=made, dst_ref=got_s.at[t, block, pl.ds(axis * part, part)], send_sem=send_sem.at[axis, k, hop, t],
            recv_sem=recv_sem.at[axis, k, hop, t], device_id={"sp": along(1 - axis, hop)}, device_id_type=MESH)

    def place(k):
        return lax.div(k, 2) * (k - 1) - lax.rem(k, 2) * (1 - lax.div(k, 2))

    def project(places, tensors):
        @pl.loop(0, 2 * side)
        def _(i):
            axis = lax.rem(i, 2) if tensors == (2,) else lax.div(i, side)
            hop = lax.div(i, 2) if tensors == (2,) else lax.rem(i, side)
            hop = hop + lax.div(hop, 2) * (5 - 2 * hop)

            if places[0] == 0:
                @pl.when((axis == 0) | (hop > 0))
                def _():
                    for t in tensors:
                        at_slot = t * slots + slot(axis, hop)
                        pltpu.make_async_copy(wo_ref.at[pl.ds(0, d), pl.ds(0, HEAD)], w_s.at[at_slot], w_sem.at[at_slot]).wait()

            here = pl.ds(pl.multiple_of(axis * part, part), part)
            c0, s0 = cos_s[here], sin_s[here]
            blocks = [along(axis, place(k)) for k in places]
            turns = [(cos_ref[pl.ds(2 * FINE + block, 1)], sin_ref[pl.ds(2 * FINE + block, 1)]) for block in blocks]
            c = jnp.concatenate([c1 * c0 - s1 * s0 for c1, s1 in turns], 0)
            sn = jnp.concatenate([s1 * c0 + c1 * s0 for c1, s1 in turns], 0)
            normed = a_s[axis, places[0] : places[-1] + 1].reshape(len(places) * part, d)
            room = lax.max(hop - 1, 0)

            def spot(k, t):
                return ask_s.at[axis, k, room] if t == 2 else made_s.at[axis, k % (side - 1), room, t]

            for t in tensors:
                made = _dot(normed, w_s[t * slots + slot(axis, hop)], 1, 0).astype(jnp.bfloat16)
                if t != 1:
                    made = made.astype(jnp.float32)
                    u, v = made[:, :half], made[:, half:]
                    made = jnp.concatenate([u * c - v * sn, v * c + u * sn], -1).astype(jnp.bfloat16)
                for i, k in enumerate(places):
                    spot(k, t)[...] = made[i * part : (i + 1) * part]

            @pl.when(hop == 0)
            def _():
                for k, block in zip(places, blocks):
                    for t in tensors:
                        got_s[t, block, here] = spot(k, t)[...]

            @pl.when(hop > 0)
            def _():
                for k in places:
                    for t in tensors:
                        send(axis, k, hop, t).start()

    project((0,), (0, 1))
    for axis, way in ways:
        spread(axis, way).wait_recv()
        relay(axis, way).start()
    project((1, 2), (0, 1))
    for axis, way in ways:
        relay(axis, way).wait_recv()

    def sent(k, tensors):
        for axis in range(2):
            @pl.loop(1, side)
            def _(hop, axis=axis):
                for t in tensors:
                    send(axis, k, hop, t).wait_send()

    sent(0, (0, 1))
    project((3,), (0, 1))
    project(tuple(range(side)), (2,))

    def fetch_wo(h, i):
        rows = pl.ds(pl.multiple_of(h * HEAD, HEAD), HEAD)
        return pltpu.make_async_copy(wo_ref.at[rows, pl.ds(i * HEAD, HEAD)], w_s.at[h, pl.ds(i * HEAD, HEAD)], wo_sem.at[h, i])

    @pl.loop(0, n)
    def _(h):
        for i in range(d // HEAD):
            fetch_wo(h, i).start()

    @pl.loop(0, 2 * side)
    def _(g):
        @pl.loop(1, side)
        def _(hop):
            for t in range(2):
                send(lax.rem(g, 2), lax.div(g, 2), hop, t).wait_recv()

    def back(j, h):
        return pltpu.make_async_remote_copy(src_ref=got_s.at[2, j], dst_ref=seen_s.at[h], send_sem=back_send.at[j], recv_sem=back_recv.at[h],
                                            device_id={"sp": j}, device_id_type=MESH)

    def pair(s, sign):
        r, end = lax.rem(s, 3), lax.div(s, 6)
        dx = (1 + 2 * r - 3 * lax.div(r, 2)) * (1 - end)
        other = lax.rem(lax.div(s, 3) + end * (side * 2 - 1 - s), 2)
        return lax.rem(mx + sign * dx + side, side) * side + 2 * lax.rem(lax.div(my, 2) + other, side // 2)

    def await_queries(block):
        dx, dy = lax.rem(lax.div(block, side) - mx + side, side), lax.rem(lax.rem(block, side) - my + side, side)
        for axis, here, there in ((0, dx, dy), (1, dy, dx)):
            hop = lax.rem(side - there, side)

            @pl.when(hop > 0)
            def _():
                send(axis, lax.rem(2 * here - lax.div(here, 2), side), hop, 2).wait_recv()

    def attend(j):
        rows = 2 * own
        q = got_s[2, pl.ds(j, 2)].reshape(rows, HEAD)
        whole, twos, odd = lax.div(j, 2), lax.div(j, 4), lax.rem(lax.div(j, 2), 2)

        def keys(t, c):
            return got_s[t, pl.ds(2 * c, 2)].reshape(PIECE, HEAD)

        def score(c, top, masked=False):
            got = _dot(q, keys(0, c), 1, 1)
            if masked:
                got = jnp.where(lax.broadcasted_iota(jnp.int32, (rows, PIECE), 0) >= lax.broadcasted_iota(jnp.int32, (rows, PIECE), 1), got, -jnp.inf)
            score_s[c] = got
            for x in range(0, PIECE, 128):
                top = jnp.maximum(top, got[:, x : x + 128])
            return top

        top = jnp.full((rows, 128), -jnp.inf, jnp.float32)
        top = lax.fori_loop(0, twos, lambda c, top: score(2 * c + 1, score(2 * c, top)), top)
        top = lax.fori_loop(2 * twos, whole, score, top)
        top = jnp.max(score(whole, top, True), axis=1, keepdims=True)

        def weigh(c, carry):
            total, mix = carry
            p = jnp.exp2((score_s[c] - top) * e)
            for x in range(0, PIECE, 128):
                total = total + p[:, x : x + 128]
            return total, mix + _dot(p.astype(jnp.bfloat16), keys(1, c), 1, 0)

        carry = jnp.zeros((rows, 128), jnp.float32), jnp.zeros((rows, HEAD), jnp.float32)
        carry = lax.fori_loop(0, twos, lambda c, carry: weigh(2 * c + 1, weigh(2 * c, carry)), carry)
        total, mix = lax.fori_loop(2 * twos, whole + 1, weigh, carry)
        out = mix / jnp.sum(total, axis=1, keepdims=True)
        got_s[2, pl.ds(j, 2)] = out.astype(jnp.bfloat16).reshape(2, own, HEAD)

    @pl.loop(0, n // 2)
    def _(s):
        j = pair(s, 1)
        for i in range(2):
            await_queries(j + i)
        attend(j)

        for i in range(2):
            @pl.when(j + i != me)
            def _():
                back(j + i, me).start()

    seen_s[me] = got_s[2, me]
    for i in range(d // PIECE):
        score_s[i, :own] = y_ref[:, i * PIECE : (i + 1) * PIECE].astype(jnp.float32)

    @pl.loop(0, n)
    def _(h):
        for i in range(d // HEAD):
            fetch_wo(h, i).wait()

    @pl.loop(0, n // 2)
    def _(s):
        h = pair(s, -1)
        for i in range(2):
            @pl.when(h + i != me)
            def _():
                back(me, h + i).wait_recv()

        for i in range(0, d, HEAD):
            score_s[i // PIECE, :own, i % PIECE : i % PIECE + HEAD] += _dot(seen_s[h], w_s[h, i : i + HEAD], 1, 0) + _dot(seen_s[h + 1], w_s[h + 1, i : i + HEAD], 1, 0)

    for i in range(d // PIECE):
        y_ref[:, i * PIECE : (i + 1) * PIECE] = score_s[i, :own].astype(jnp.bfloat16)

    for axis, way in ways:
        spread(axis, way).wait_send()
        relay(axis, way).wait_send()

    for k in range(side):
        sent(k, (0, 1, 2) if k else (2,))

    @pl.loop(0, n)
    def _(j):
        @pl.when(j != me)
        def _():
            back(j, me).wait_send()


def solution(mesh):
    n = mesh.shape["sp"]
    side = math.isqrt(n)

    def step(x, gain, wq, wk, wv, wo):
        own, d = x.shape
        half = HEAD // 2
        place = jnp.concatenate([jnp.arange(FINE), jnp.arange(FINE) * FINE, jnp.arange(n) * own])
        angle = place.astype(jnp.float32)[:, None] * THETA ** (-jnp.arange(half, dtype=jnp.float32) / half)
        vmem, hbm = pl.BlockSpec(memory_space=pltpu.VMEM), pl.BlockSpec(memory_space=pl.ANY)
        low, wide, dma = jnp.bfloat16, jnp.float32, pltpu.SemaphoreType.DMA
        slots = 3 * (2 * side - 1)
        return pl.pallas_call(
            functools.partial(_kernel, n),
            out_shape=pltpu.VMEM((own, d), low),
            in_specs=[hbm] + [vmem] * 3 + [hbm] * 4,
            out_specs=vmem,
            scratch_shapes=[
                pltpu.VMEM((2, side, own // 2, d), low),
                pltpu.VMEM((slots, d, HEAD), low),
                pltpu.VMEM((2, side - 1, side - 1, 2, own // 2, HEAD), low),
                pltpu.VMEM((2, side, side - 1, own // 2, HEAD), low),
                pltpu.VMEM((3, n, own, HEAD), low),
                pltpu.VMEM((n * own // PIECE, 2 * own, PIECE), wide),
                pltpu.VMEM((n, own, HEAD), low),
                pltpu.VMEM((own, half), wide),
                pltpu.VMEM((own, half), wide),
                dma((1,)),
                dma((slots,)),
                dma((2, 4)),
                dma((2, 4)),
                dma((2, side, side, 3)),
                dma((2, side, side, 3)),
                dma((n,)),
                dma((n,)),
                dma((n, d // HEAD)),
            ],
            compiler_params=pltpu.CompilerParams(collective_id=0, has_side_effects=True, vmem_limit_bytes=VMEM),
        )(x, gain, jnp.cos(angle), jnp.sin(angle), wq, wk, wv, wo)

    tokens, whole = P(("dp", "sp"), None), P(None, None)
    return jax.shard_map(
        step,
        mesh=mesh,
        in_specs=(tokens, P(None), whole, whole, whole, whole),
        out_specs=tokens,
        check_vma=False,
    )
```

```python
import functools
import math

import jax
import jax.numpy as jnp
from jax import lax
from jax.experimental import pallas as pl
from jax.experimental.pallas import tpu as pltpu
from jax.sharding import PartitionSpec as P

HEAD = 256
THETA = 10000
LOG2E = 1.4426950408889634
MESH = pl.DeviceIdType.MESH
VMEM = 65_470_000
PIECE = 512
FINE = 16


def _dot(a, b, ca, cb):
    return lax.dot_general(a, b, (((ca,), (cb,)), ((), ())), preferred_element_type=jnp.float32)


def _kernel(n, x_ref, gain_ref, cos_ref, sin_ref, wq_ref, wk_ref, wv_ref, wo_ref, y_ref,
            a_s, w_s, made_s, ask_s, got_s, score_s, seen_s, cos_s, sin_s,
            x_sem, w_sem, a_send, a_recv, send_sem, recv_sem, back_send, back_recv, wo_sem):
    side = math.isqrt(n)
    me = lax.axis_index("sp")
    mx, my = lax.div(me, side), lax.rem(me, side)
    own, d = x_ref.shape
    part = own // 2
    e = HEAD**-0.5 * LOG2E
    half = HEAD // 2

    def go(dx, dy):
        return lax.rem(mx + dx + side, side) * side + lax.rem(my + dy + side, side)

    def along(axis, hop):
        return go(hop * (1 - axis), hop * axis)

    def at(s, sign):
        dx = lax.rem(s, side)
        return go(sign * dx, sign * lax.rem(lax.div(s, side) + dx, side))

    take_x = pltpu.make_async_copy(x_ref, y_ref, x_sem.at[0])
    take_x.start()
    barrier = pltpu.get_barrier_semaphore()

    @pl.loop(1, n)
    def _(s):
        pl.semaphore_signal(barrier, inc=1, device_id={"sp": at(s, 1)}, device_id_type=MESH)

    slots = 2 * side - 1

    def slot(axis, hop):
        return hop + axis * (side - 1) * lax.min(hop, 1)

    def fetch(t, i):
        head = along(1, i) if i < side else along(0, i - side + 1)
        columns = pl.ds(pl.multiple_of(head * HEAD, HEAD), HEAD)
        return pltpu.make_async_copy((wk_ref, wv_ref, wq_ref)[t].at[:, columns], w_s.at[t * slots + i], w_sem.at[t * slots + i])

    for tensors in ((0, 1), (2,)):
        for i in (0, *range(1, side - 2), side - 1, side - 2, *range(side, slots)):
            for t in tensors:
                fetch(t, i).start()

    take_x.wait()
    gain = gain_ref[...].astype(jnp.float32).reshape(1, d)

    @pl.loop(0, own // FINE)
    def _(i):
        wide = y_ref[pl.ds(pl.multiple_of(i * FINE, FINE), FINE)].astype(jnp.float32)
        scale = lax.rsqrt(jnp.mean(wide * wide, -1, keepdims=True) + 1e-6)
        at_row = lax.rem(i, part // FINE) * FINE
        a_s[lax.div(i, part // FINE), 0, pl.ds(pl.multiple_of(at_row, FINE), FINE)] = (wide * scale * gain).astype(jnp.bfloat16)

    pl.semaphore_wait(barrier, n - 1)

    def spread(axis, way):
        return pltpu.make_async_remote_copy(
            src_ref=a_s.at[axis, 0], dst_ref=a_s.at[axis, 1 + way], send_sem=a_send.at[axis, way], recv_sem=a_recv.at[axis, way],
            device_id={"sp": along(axis, 1 - 2 * way)}, device_id_type=MESH)

    def relay(axis, way):
        rows = pl.ds(way * (part // 2), part // 2)
        return pltpu.make_async_remote_copy(
            src_ref=a_s.at[axis, 1 + way, rows], dst_ref=a_s.at[axis, 3, rows], send_sem=a_send.at[axis, 2 + way],
            recv_sem=a_recv.at[axis, 2 + way], device_id={"sp": along(axis, 1 - 2 * way)}, device_id_type=MESH)

    ways = [(axis, way) for way in range(2) for axis in range(2)]
    for axis, way in ways:
        spread(axis, way).start()

    for i in range(own // FINE):
        rows = slice(i * FINE, (i + 1) * FINE)
        c1, s1, c0, s0 = cos_ref[FINE + i : FINE + i + 1], sin_ref[FINE + i : FINE + i + 1], cos_ref[:FINE], sin_ref[:FINE]
        cos_s[rows] = c1 * c0 - s1 * s0
        sin_s[rows] = s1 * c0 + c1 * s0

    def send(axis, k, hop, t):
        block = along(axis, place(k))
        made = ask_s.at[axis, k, hop - 1] if t == 2 else made_s.at[axis, lax.rem(k, side - 1), hop - 1, t]
        return pltpu.make_async_remote_copy(
            src_ref=made, dst_ref=got_s.at[t, block, pl.ds(axis * part, part)], send_sem=send_sem.at[axis, k, hop, t],
            recv_sem=recv_sem.at[axis, k, hop, t], device_id={"sp": along(1 - axis, hop)}, device_id_type=MESH)

    def place(k):
        return lax.div(k, 2) * (k - 1) - lax.rem(k, 2) * (1 - lax.div(k, 2))

    def project(places, tensors):
        @pl.loop(0, 2 * side)
        def _(i):
            axis = lax.rem(i, 2) if tensors == (2,) else lax.div(i, side)
            hop = lax.div(i, 2) if tensors == (2,) else lax.rem(i, side)
            hop = hop + lax.div(hop, 2) * (5 - 2 * hop)

            if places[0] == 0:
                @pl.when((axis == 0) | (hop > 0))
                def _():
                    for t in tensors:
                        at_slot = t * slots + slot(axis, hop)
                        pltpu.make_async_copy(wo_ref.at[pl.ds(0, d), pl.ds(0, HEAD)], w_s.at[at_slot], w_sem.at[at_slot]).wait()

            here = pl.ds(pl.multiple_of(axis * part, part), part)
            c0, s0 = cos_s[here], sin_s[here]
            blocks = [along(axis, place(k)) for k in places]
            turns = [(cos_ref[pl.ds(2 * FINE + block, 1)], sin_ref[pl.ds(2 * FINE + block, 1)]) for block in blocks]
            c = jnp.concatenate([c1 * c0 - s1 * s0 for c1, s1 in turns], 0)
            sn = jnp.concatenate([s1 * c0 + c1 * s0 for c1, s1 in turns], 0)
            normed = a_s[axis, places[0] : places[-1] + 1].reshape(len(places) * part, d)
            room = lax.max(hop - 1, 0)

            def spot(k, t):
                return ask_s.at[axis, k, room] if t == 2 else made_s.at[axis, k % (side - 1), room, t]

            for t in tensors:
                made = _dot(normed, w_s[t * slots + slot(axis, hop)], 1, 0).astype(jnp.bfloat16)
                if t != 1:
                    made = made.astype(jnp.float32)
                    u, v = made[:, :half], made[:, half:]
                    made = jnp.concatenate([u * c - v * sn, v * c + u * sn], -1).astype(jnp.bfloat16)
                for i, k in enumerate(places):
                    spot(k, t)[...] = made[i * part : (i + 1) * part]

            @pl.when(hop == 0)
            def _():
                for k, block in zip(places, blocks):
                    for t in tensors:
                        got_s[t, block, here] = spot(k, t)[...]

            @pl.when(hop > 0)
            def _():
                for k in places:
                    for t in tensors:
                        send(axis, k, hop, t).start()

    project((0,), (0, 1))
    for axis, way in ways:
        spread(axis, way).wait_recv()
        relay(axis, way).start()
    project((1, 2), (0, 1))
    for axis, way in ways:
        relay(axis, way).wait_recv()

    def sent(k, tensors):
        for axis in range(2):
            @pl.loop(1, side)
            def _(hop, axis=axis):
                for t in tensors:
                    send(axis, k, hop, t).wait_send()

    sent(0, (0, 1))
    project((3,), (0, 1))
    project(tuple(range(side)), (2,))

    def fetch_wo(h, i):
        rows = pl.ds(pl.multiple_of(h * HEAD, HEAD), HEAD)
        return pltpu.make_async_copy(wo_ref.at[rows, pl.ds(i * HEAD, HEAD)], w_s.at[h, pl.ds(i * HEAD, HEAD)], wo_sem.at[h, i])

    @pl.loop(0, n)
    def _(h):
        for i in range(d // HEAD):
            fetch_wo(h, i).start()

    @pl.loop(0, 2 * side)
    def _(g):
        @pl.loop(1, side)
        def _(hop):
            for t in range(2):
                send(lax.rem(g, 2), lax.div(g, 2), hop, t).wait_recv()

    def back(j, h):
        return pltpu.make_async_remote_copy(src_ref=got_s.at[2, j], dst_ref=seen_s.at[h], send_sem=back_send.at[j], recv_sem=back_recv.at[h],
                                            device_id={"sp": j}, device_id_type=MESH)

    def pair(s, sign):
        r, end = lax.rem(s, 3), lax.div(s, 6)
        dx = (1 + 2 * r - 3 * lax.div(r, 2)) * (1 - end)
        other = lax.rem(lax.div(s, 3) + end * (side * 2 - 1 - s), 2)
        return lax.rem(mx + sign * dx + side, side) * side + 2 * lax.rem(lax.div(my, 2) + other, side // 2)

    def await_queries(block):
        dx, dy = lax.rem(lax.div(block, side) - mx + side, side), lax.rem(lax.rem(block, side) - my + side, side)
        for axis, here, there in ((0, dx, dy), (1, dy, dx)):
            hop = lax.rem(side - there, side)

            @pl.when(hop > 0)
            def _():
                send(axis, lax.rem(2 * here - lax.div(here, 2), side), hop, 2).wait_recv()

    def attend(j):
        rows = 2 * own
        q = got_s[2, pl.ds(j, 2)].reshape(rows, HEAD)
        whole, twos = lax.div(j, 2), lax.div(j, 4)

        def keys(t, c):
            return got_s[t, pl.ds(2 * c, 2)].reshape(PIECE, HEAD)

        def score(c, top, masked=False):
            got = _dot(q, keys(0, c), 1, 1)
            if masked:
                got = jnp.where(lax.broadcasted_iota(jnp.int32, (rows, PIECE), 0) >= lax.broadcasted_iota(jnp.int32, (rows, PIECE), 1), got, -jnp.inf)
            score_s[c] = got
            for x in range(0, PIECE, 128):
                top = jnp.maximum(top, got[:, x : x + 128])
            return top

        top = jnp.full((rows, 128), -jnp.inf, jnp.float32)
        top = lax.fori_loop(0, twos, lambda c, top: score(2 * c + 1, score(2 * c, top)), top)
        top = lax.fori_loop(2 * twos, whole, score, top)
        top = jnp.max(score(whole, top, True), axis=1, keepdims=True)

        def weigh(c, carry):
            total, mix = carry
            p = jnp.exp2((score_s[c] - top) * e)
            for x in range(0, PIECE, 128):
                total = total + p[:, x : x + 128]
            return total, mix + _dot(p.astype(jnp.bfloat16), keys(1, c), 1, 0)

        carry = jnp.zeros((rows, 128), jnp.float32), jnp.zeros((rows, HEAD), jnp.float32)
        twos = lax.div(whole + 1, 2)
        carry = lax.fori_loop(0, twos, lambda c, carry: weigh(2 * c + 1, weigh(2 * c, carry)), carry)
        total, mix = lax.fori_loop(2 * twos, whole + 1, weigh, carry)
        out = mix / jnp.sum(total, axis=1, keepdims=True)
        got_s[2, pl.ds(j, 2)] = out.astype(jnp.bfloat16).reshape(2, own, HEAD)

    @pl.loop(0, n // 2)
    def _(s):
        j = pair(s, 1)
        for i in range(2):
            await_queries(j + i)
        attend(j)

        for i in range(2):
            @pl.when(j + i != me)
            def _():
                back(j + i, me).start()

    seen_s[me] = got_s[2, me]
    for i in range(d // PIECE):
        score_s[i, :own] = y_ref[:, i * PIECE : (i + 1) * PIECE].astype(jnp.float32)

    @pl.loop(0, n)
    def _(h):
        for i in range(d // HEAD):
            fetch_wo(h, i).wait()

    @pl.loop(0, n // 2)
    def _(s):
        h = pair(s, -1)
        for i in range(2):
            @pl.when(h + i != me)
            def _():
                back(me, h + i).wait_recv()

        for i in range(0, d, HEAD):
            score_s[i // PIECE, :own, i % PIECE : i % PIECE + HEAD] += _dot(seen_s[h], w_s[h, i : i + HEAD], 1, 0) + _dot(seen_s[h + 1], w_s[h + 1, i : i + HEAD], 1, 0)

    for i in range(d // PIECE):
        y_ref[:, i * PIECE : (i + 1) * PIECE] = score_s[i, :own].astype(jnp.bfloat16)

    for axis, way in ways:
        spread(axis, way).wait_send()
        relay(axis, way).wait_send()

    for k in range(side):
        sent(k, (0, 1, 2) if k else (2,))

    @pl.loop(0, n)
    def _(j):
        @pl.when(j != me)
        def _():
            back(j, me).wait_send()


def solution(mesh):
    n = mesh.shape["sp"]
    side = math.isqrt(n)

    def step(x, gain, wq, wk, wv, wo):
        own, d = x.shape
        half = HEAD // 2
        place = jnp.concatenate([jnp.arange(FINE), jnp.arange(FINE) * FINE, jnp.arange(n) * own])
        angle = place.astype(jnp.float32)[:, None] * THETA ** (-jnp.arange(half, dtype=jnp.float32) / half)
        vmem, hbm = pl.BlockSpec(memory_space=pltpu.VMEM), pl.BlockSpec(memory_space=pl.ANY)
        low, wide, dma = jnp.bfloat16, jnp.float32, pltpu.SemaphoreType.DMA
        slots = 3 * (2 * side - 1)
        return pl.pallas_call(
            functools.partial(_kernel, n),
            out_shape=pltpu.VMEM((own, d), low),
            in_specs=[hbm] + [vmem] * 3 + [hbm] * 4,
            out_specs=vmem,
            scratch_shapes=[
                pltpu.VMEM((2, side, own // 2, d), low),
                pltpu.VMEM((slots, d, HEAD), low),
                pltpu.VMEM((2, side - 1, side - 1, 2, own // 2, HEAD), low),
                pltpu.VMEM((2, side, side - 1, own // 2, HEAD), low),
                pltpu.VMEM((3, n, own, HEAD), low),
                pltpu.VMEM((n * own // PIECE, 2 * own, PIECE), wide),
                pltpu.VMEM((n, own, HEAD), low),
                pltpu.VMEM((own, half), wide),
                pltpu.VMEM((own, half), wide),
                dma((1,)),
                dma((slots,)),
                dma((2, 4)),
                dma((2, 4)),
                dma((2, side, side, 3)),
                dma((2, side, side, 3)),
                dma((n,)),
                dma((n,)),
                dma((n, d // HEAD)),
            ],
            compiler_params=pltpu.CompilerParams(collective_id=0, has_side_effects=True, vmem_limit_bytes=VMEM),
        )(x, gain, jnp.cos(angle), jnp.sin(angle), wq, wk, wv, wo)

    tokens, whole = P(("dp", "sp"), None), P(None, None)
    return jax.shard_map(
        step,
        mesh=mesh,
        in_specs=(tokens, P(None), whole, whole, whole, whole),
        out_specs=tokens,
        check_vma=False,
    )
```
